32 devices in a mesh: rep: 1, dp: 32 (over x, y, z, core).
Axes of the slice: x: 2, y: 2, z: 4, core: 2. Of those that a mesh axis runs over, the one named last changes fastest.
Arguments:
- g_w_gate: bfloat16 [32, 2, 512, 8192], P(('rep', 'dp'))
- g_w_up: bfloat16 [32, 2, 512, 8192], P(('rep', 'dp'))
- g_w_down: bfloat16 [32, 2, 8192, 512], P(('rep', 'dp'))
- w_gate: bfloat16 [2, 512, 8192], replicated
- w_up: bfloat16 [2, 512, 8192], replicated
- w_down: bfloat16 [2, 8192, 512], replicated
- m_w_gate: float32 [2, 512, 8192], P(None, 'dp')
- m_w_up: float32 [2, 512, 8192], P(None, 'dp')
- m_w_down: float32 [2, 8192, 512], P(None, 'dp')
- v_w_gate: float32 [2, 512, 8192], P(None, 'dp')
- v_w_up: float32 [2, 512, 8192], P(None, 'dp')
- v_w_down: float32 [2, 8192, 512], P(None, 'dp')
Outputs:
- output 1: bfloat16 [2, 512, 8192], P('rep')
- output 2: bfloat16 [2, 512, 8192], P('rep')
- output 3: bfloat16 [2, 8192, 512], P('rep')
- output 4: float32 [2, 512, 8192], P('rep', 'dp')
- output 5: float32 [2, 512, 8192], P('rep', 'dp')
- output 6: float32 [2, 8192, 512], P('rep', 'dp')
- output 7: float32 [2, 512, 8192], P('rep', 'dp')
- output 8: float32 [2, 512, 8192], P('rep', 'dp')
- output 9: float32 [2, 8192, 512], P('rep', 'dp')
All inputs are finite; a program needn't handle non-finite values.
Results may differ from the reference program's by a relative error of at most 0.022.
Values are sent between devices in bfloat16 or wider.
A program may use at most 2 GiB of HBM per device.

```python
import jax
import jax.numpy as jnp
from jax import lax

DEVICES = 32
D = 512
FF = 8192
LAYERS = 2
NAMES = ("w_gate", "w_up", "w_down")
SHAPES = {"w_gate": (LAYERS, D, FF), "w_up": (LAYERS, D, FF), "w_down": (LAYERS, FF, D)}


def setup_inputs(seed: int = 0, part: int = 0) -> dict:
    kz, *keys = jax.random.split(jax.random.key(seed), 1 + 5 * len(NAMES))
    loud = 2.0 ** jax.random.uniform(kz, (), jnp.float32, -1.0, 1.0)
    drawn = {}
    for name, key, both in zip(NAMES, keys[:3], keys[3:6], strict=True):
        own = jax.random.normal(jax.random.fold_in(key, part), (DEVICES, *SHAPES[name]), jnp.float32)
        shared = jax.random.normal(jax.random.fold_in(both, part), SHAPES[name], jnp.float32)
        drawn["g_" + name] = (loud * (0.7 * shared / DEVICES + 0.7 * own * DEVICES**-0.5)).astype(jnp.bfloat16)
    for name, key in zip(NAMES, keys[6:9], strict=True):
        drawn[name] = (jax.random.normal(key, SHAPES[name], jnp.float32) * SHAPES[name][1] ** -0.5).astype(jnp.bfloat16)
    for name, key in zip(NAMES, keys[9:12], strict=True):
        drawn["m_" + name] = loud * 0.5 * jax.random.normal(key, SHAPES[name], jnp.float32)
    for name, key in zip(NAMES, keys[12:15], strict=True):
        drawn["v_" + name] = loud * loud * jax.random.uniform(key, SHAPES[name], jnp.float32, 0.5, 1.5)
    return drawn


def adamw(w, m, v, g):
    m = 0.9 * m + 0.1 * g
    v = 0.95 * v + 0.05 * g * g
    step = m * lax.rsqrt(v + 1e-8) + 0.1 * w
    return (w - 0.02 * step).astype(jnp.bfloat16), m, v


def reference(g_w_gate, g_w_up, g_w_down, w_gate, w_up, w_down, m_w_gate, m_w_up, m_w_down, v_w_gate, v_w_up, v_w_down):
    def total(terms):
        return lax.scan(lambda so_far, term: (so_far + term.astype(jnp.float32), None), jnp.zeros(terms.shape[1:], jnp.float32), terms)[0]

    gradients = [total(terms).astype(jnp.bfloat16).astype(jnp.float32) for terms in (g_w_gate, g_w_up, g_w_down)]
    new = [
        adamw(w.astype(jnp.float32), m, v, g)
        for w, m, v, g in zip((w_gate, w_up, w_down), (m_w_gate, m_w_up, m_w_down), (v_w_gate, v_w_up, v_w_down), gradients, strict=True)
    ]
    return tuple(one[which] for which in range(3) for one in new)
```

```python
import functools

import jax
import jax.numpy as jnp
from jax import lax
from jax.experimental import pallas as pl
from jax.experimental.pallas import tpu as pltpu
from jax.sharding import PartitionSpec as P

F32, BF16 = jnp.float32, jnp.bfloat16
UNIT = 512

UNITS = 2
PER_LAYER = 16 // UNITS
CHUNKS = 6 * PER_LAYER

S1 = 1
T = S1 + 2
LZ = 1
FIN = T + 3 * LZ
NEW = FIN + 1
GZ = NEW + 2
G1 = GZ + 3 * LZ
G0 = G1 + 2
END = G0 + 2

SLOTS = 32
EARLY = 16
OWN = 4
SUMS = 8


def kernel(*refs):
    g, w, m, v, out, m_out, v_out = (refs[i : i + 3] for i in range(0, 21, 3))
    own, core, first, zs, last, last_send, new, sums, kept, wb, mb, vb, mo, vo, local, recv, zrecv, grecv, sent, stored = refs[21:]

    rep, me = lax.axis_index("rep"), lax.axis_index("dp")
    c, z, y, x = lax.rem(me, 2), lax.rem(lax.div(me, 2), 4), lax.rem(lax.div(me, 8), 2), lax.div(me, 16)
    other = me + 1 - 2 * c
    xn, yn = me + 16 * (1 - 2 * x), me + 8 * (1 - 2 * y)

    def order(k):
        odd = lax.rem(k, 2)
        pn, qn = xn + odd * (yn - xn), yn + odd * (xn - yn)
        p, q = x + odd * (y - x), y + odd * (x - y)
        return pn, qn, p, q, 8 - 4 * odd, 4 + 4 * odd

    def by_weight(k, body):
        at = lax.div(k, PER_LAYER)
        which, layer, piece = lax.div(at, 2), lax.rem(at, 2), lax.rem(k, PER_LAYER)
        for i in range(3):
            pl.when(which == i)(functools.partial(body, i, layer, piece))

    def cut(i, piece, u=None):
        start, n = (piece * UNITS, UNITS) if u is None else (piece * UNITS + u, 1)
        if i < 2:
            return slice(None), pl.ds(pl.multiple_of(start * UNIT, UNIT), n * UNIT)
        return pl.ds(pl.multiple_of(start * 16, 16), n * 16), slice(None)

    def send(src, dst, s, r, to):
        pltpu.make_async_remote_copy(src, dst, s, r, device_id=(rep, to), device_id_type=pl.DeviceIdType.MESH).start()

    def wait(like, sem):
        pltpu.make_async_copy(like, like, sem).wait()

    def stage(t, offset, body):
        k = t - offset
        pl.when(jnp.logical_and(k >= 0, k < CHUNKS))(functools.partial(body, k))

    CORE, FIRST, LAST, NEXT, GATHER1, GATHER0, GATHERZ = range(7)

    def start(k):
        s, e, o = lax.rem(k, SLOTS), lax.rem(k, EARLY), lax.rem(k, OWN)

        def body(i, layer, piece):
            for u in range(UNITS):
                rows, cols = cut(i, piece, u)
                send(g[i].at[layer, :, 1 - c, rows, cols], core.at[e, :, u], sent.at[CORE, s], recv.at[CORE, s], other)
                pltpu.make_async_copy(g[i].at[layer, :, c, rows, cols], own.at[o, :, u], local.at[o]).start()

        by_weight(k, body)

    def first_axis(k):
        s, e, o = lax.rem(k, SLOTS), lax.rem(k, EARLY), lax.rem(k, OWN)
        pn, _, p, _, sp, sq = order(k)
        wait(core.at[e], recv.at[CORE, s])
        wait(own.at[o], local.at[o])
        for q in range(2):
            j = (1 - p) * sp + q * sq

            @pl.loop(0, 4)
            def _(n):
                core[e, j + n] = (own[o, j + n].astype(F32) + core[e, j + n].astype(F32)).astype(BF16)

            send(core.at[e, pl.ds(j, 4)], first.at[e, q], sent.at[FIRST, s], recv.at[FIRST, s], pn)

    def sum_first(k):
        s, e, o, b = lax.rem(k, SLOTS), lax.rem(k, EARLY), lax.rem(k, OWN), lax.rem(k, SUMS)
        _, _, p, _, sp, sq = order(k)
        wait(first.at[e], recv.at[FIRST, s])
        for q in range(2):
            j = p * sp + q * sq

            @pl.loop(0, 4)
            def _(n):
                sums[b, n, q] = own[o, j + n].astype(F32) + core[e, j + n].astype(F32) + first[e, q, n].astype(F32)

    def hop(k, up):
        s, b = lax.rem(k, SLOTS), lax.rem(k, SUMS)
        for to in (3, 2, 1) if up else (0, 1, 2):
            slot = to + 1 if up else to

            @pl.when(to > z if up else to < z)
            def _():
                @pl.when(z > 0 if up else z < 3)
                def _():
                    wait(zs.at[s, slot], zrecv.at[s, slot])
                    for q in range(2):
                        zs[s, slot, q] = (sums[b, to, q] + zs[s, slot, q].astype(F32)).astype(BF16)

                @pl.when(z == 0 if up else z == 3)
                def _():
                    for q in range(2):
                        zs[s, slot, q] = sums[b, to, q].astype(BF16)

                send(zs.at[s, slot], zs.at[s, slot], sent.at[GATHERZ + 1, s], zrecv.at[s, slot], me + 2 if up else me - 2)

    def finish(k):
        s, b, h = lax.rem(k, SLOTS), lax.rem(k, SUMS), lax.rem(k, 2)
        _, qn, _, q, _, _ = order(k)

        @pl.when(z > 0)
        def _():
            wait(zs.at[s, z + 1], zrecv.at[s, z + 1])

        @pl.when(z < 3)
        def _():
            wait(zs.at[s, z], zrecv.at[s, z])

        def total(at):
            return sums[b, z, at]

        @pl.when(z == 0)
        def _():
            last_send[s] = (sums[b, z, 1 - q] + zs[s, z, 1 - q].astype(F32)).astype(BF16)
            kept[h] = sums[b, z, q] + zs[s, z, q].astype(F32)

        @pl.when(z == 3)
        def _():
            last_send[s] = (sums[b, z, 1 - q] + zs[s, z + 1, 1 - q].astype(F32)).astype(BF16)
            kept[h] = sums[b, z, q] + zs[s, z + 1, q].astype(F32)

        @pl.when(jnp.logical_and(z > 0, z < 3))
        def _():
            last_send[s] = (sums[b, z, 1 - q] + zs[s, z, 1 - q].astype(F32) + zs[s, z + 1, 1 - q].astype(F32)).astype(BF16)
            kept[h] = sums[b, z, q] + zs[s, z, q].astype(F32) + zs[s, z + 1, q].astype(F32)

        send(last_send.at[s], last.at[s], sent.at[LAST, s], recv.at[LAST, s], qn)

        def load(i, layer, piece):
            for u in range(UNITS):
                rows, cols = cut(i, piece, u)
                pltpu.make_async_copy(w[i].at[layer, me, rows, cols], wb.at[h, u], local.at[OWN + h]).start()
                pltpu.make_async_copy(m[i].at[layer, rows, cols], mb.at[h, u], local.at[OWN + 2 + h]).start()
                pltpu.make_async_copy(v[i].at[layer, rows, cols], vb.at[h, u], local.at[OWN + 4 + h]).start()

        by_weight(k, load)

    def wait_stored(h):
        wait(mo.at[h], stored.at[h])
        wait(vo.at[h], stored.at[2 + h])

    def update(k):
        s, h = lax.rem(k, SLOTS), lax.rem(k, 2)
        _, qn, _, _, _, _ = order(k)
        wait(last.at[s], recv.at[LAST, s])
        wait(wb.at[h], local.at[OWN + h])
        wait(mb.at[h], local.at[OWN + 2 + h])
        wait(vb.at[h], local.at[OWN + 4 + h])
        pl.when(k >= 2)(functools.partial(wait_stored, h))
        grad = (kept[h] + last[s].astype(F32)).astype(BF16).astype(F32)
        old = wb[h].astype(F32)
        mm = 0.9 * mb[h] + 0.1 * grad
        vv = 0.95 * vb[h] + 0.05 * grad * grad
        mo[h] = mm
        vo[h] = vv
        new[s] = (old - 0.02 * (mm * lax.rsqrt(vv + 1e-8) + 0.1 * old)).astype(BF16)

        def store(i, layer, piece):
            for u in range(UNITS):
                rows, cols = cut(i, piece, u)
                here = out[i].at[layer, lax.div(me, 2), c, rows, cols]
                send(new.at[s, u], here, sent.at[NEXT, s], recv.at[NEXT, s], qn)
                pltpu.make_async_copy(new.at[s, u], here, stored.at[4 + lax.rem(k, 4)]).start()
                pltpu.make_async_copy(mo.at[h, u], m_out[i].at[layer, rows, cols], stored.at[h]).start()
                pltpu.make_async_copy(vo.at[h, u], v_out[i].at[layer, rows, cols], stored.at[2 + h]).start()

        by_weight(k, store)

    def like(pieces):
        if pieces == 1:
            return out[0].at[0, 0, 0, :, pl.ds(0, UNITS * UNIT)]
        if pieces <= 16:
            return out[0].at[0, pl.ds(0, pieces), 0, :, pl.ds(0, UNITS * UNIT)]
        raise ValueError(pieces)

    def pass_on(k, at, up, down):
        s = lax.rem(k, SLOTS)
        _, _, p, _, sp, sq = order(k)

        def body(i, layer, piece):
            rows, cols = cut(i, piece)
            for cond, to in ((up, me + 2), (down, me - 2)):
                if cond is not None:

                    @pl.when(cond)
                    def _():
                        for q in range(2):
                            block = out[i].at[layer, p * sp + q * sq + at, c, rows, cols]
                            send(block, block, sent.at[GATHERZ, s], grecv.at[s, at], to)

        by_weight(k, body)

    def gather_own(k):
        s = lax.rem(k, SLOTS)
        wait(new.at[s], stored.at[4 + lax.rem(k, 4)])
        wait(new.at[s], recv.at[NEXT, s])
        pass_on(k, z, z < 3, z > 0)

    def gather_z(k, d):
        s = lax.rem(k, SLOTS)

        @pl.when(z - d >= 0)
        def _():
            wait(like(2), grecv.at[s, z - d])
            if d < 3:
                pass_on(k, z - d, z < 3, None)

        @pl.when(z + d <= 3)
        def _():
            wait(like(2), grecv.at[s, z + d])
            if d < 3:
                pass_on(k, z + d, None, z > 0)

    def gather_first(k):
        s = lax.rem(k, SLOTS)
        pn, _, p, _, sp, sq = order(k)

        def body(i, layer, piece):
            rows, cols = cut(i, piece)
            for q in range(2):
                block = out[i].at[layer, pl.ds(p * sp + q * sq, 4), c, rows, cols]
                send(block, block, sent.at[GATHER1, s], recv.at[GATHER1, s], pn)

        by_weight(k, body)

    def gather_core(k):
        s = lax.rem(k, SLOTS)
        wait(like(8), recv.at[GATHER1, s])

        def body(i, layer, piece):
            rows, cols = cut(i, piece)
            block = out[i].at[layer, :, c, rows, cols]
            send(block, block, sent.at[GATHER0, s], recv.at[GATHER0, s], other)

        by_weight(k, body)

    def sent_first(k):
        s, e = lax.rem(k, SLOTS), lax.rem(k, EARLY)
        wait(core.at[e], sent.at[CORE, s])
        wait(first.at[e], sent.at[FIRST, s])

    def end(k):
        s = lax.rem(k, SLOTS)
        wait(like(16), recv.at[GATHER0, s])
        wait(zs.at[s, pl.ds(0, 3)], sent.at[GATHERZ + 1, s])
        wait(last.at[s], sent.at[LAST, s])
        wait(new.at[s], sent.at[NEXT, s])
        pl.when(jnp.logical_or(z == 0, z == 3))(lambda: wait(like(2), sent.at[GATHERZ, s]))
        pl.when(jnp.logical_and(z > 0, z < 3))(lambda: wait(like(10), sent.at[GATHERZ, s]))
        wait(like(8), sent.at[GATHER1, s])
        wait(like(16), sent.at[GATHER0, s])

    @pl.loop(0, CHUNKS + END)
    def _(t):
        stage(t, END, end)
        stage(t, G0, gather_core)
        for d in (3, 2, 1):
            stage(t, GZ + d * LZ, functools.partial(gather_z, d=d))
        stage(t, G1, gather_first)
        stage(t, GZ, gather_own)
        stage(t, NEW, update)
        stage(t, T + 5, sent_first)
        stage(t, FIN, finish)
        stage(t, T, sum_first)
        stage(t, T + LZ * z, functools.partial(hop, up=True))
        stage(t, T + LZ * (3 - z), functools.partial(hop, up=False))
        stage(t, S1, first_axis)
        stage(t, 0, start)

    for h in range(2):
        wait_stored(h)


def solution(mesh):
    n = (UNITS, 16, UNIT)

    def step(*arrays):
        g, w, m, v = (arrays[i : i + 3] for i in (0, 3, 6, 9))
        shapes = [one.shape for one in w]
        g = [one.reshape(2, 16, 2, one.shape[2] // 32, one.shape[3]) for one in g]
        w = [one.reshape(2, 32, one.shape[1] // 32, one.shape[2]) for one in w]
        results = pl.pallas_call(
            kernel,
            name="step",
            in_specs=[pl.BlockSpec(memory_space=pl.ANY)] * 12,
            out_specs=[pl.BlockSpec(memory_space=pl.ANY)] * 9,
            out_shape=[jax.ShapeDtypeStruct(one.shape, BF16) for one in g] + [jax.ShapeDtypeStruct(one.shape, F32) for one in (*m, *v)],
            scratch_shapes=[
                pltpu.VMEM((OWN, 16, *n), BF16),
                pltpu.VMEM((EARLY, 16, *n), BF16),
                pltpu.VMEM((EARLY, 2, 4, *n), BF16),
                pltpu.VMEM((SLOTS, 5, 2, *n), BF16),
                pltpu.VMEM((SLOTS, *n), BF16),
                pltpu.VMEM((SLOTS, *n), BF16),
                pltpu.VMEM((SLOTS, *n), BF16),
                pltpu.VMEM((SUMS, 4, 2, *n), F32),
                pltpu.VMEM((2, *n), F32),
                pltpu.VMEM((2, *n), BF16),
                pltpu.VMEM((2, *n), F32),
                pltpu.VMEM((2, *n), F32),
                pltpu.VMEM((2, *n), F32),
                pltpu.VMEM((2, *n), F32),
                pltpu.SemaphoreType.DMA((OWN + 6,)),
                pltpu.SemaphoreType.DMA((6, SLOTS)),
                pltpu.SemaphoreType.DMA((SLOTS, 5)),
                pltpu.SemaphoreType.DMA((SLOTS, 4)),
                pltpu.SemaphoreType.DMA((8, SLOTS)),
                pltpu.SemaphoreType.DMA((8,)),
            ],
            compiler_params=pltpu.CompilerParams(has_side_effects=True, vmem_limit_bytes=67_043_328),
        )(*g, *w, *m, *v)
        return (*(one.reshape(shape) for one, shape in zip(results[:3], shapes, strict=True)), *results[3:])

    all_of, cut = P(None, None, None), P(None, "dp", None)
    return jax.shard_map(
        step,
        mesh=mesh,
        in_specs=(P(("rep", "dp"), None, None, None),) * 3 + (all_of,) * 3 + (cut,) * 6,
        out_specs=(P("rep", None, None),) * 3 + (P("rep", "dp", None),) * 6,
        check_vma=False,
    )
```

```python
import functools

import jax
import jax.numpy as jnp
from jax import lax
from jax.experimental import pallas as pl
from jax.experimental.pallas import tpu as pltpu
from jax.sharding import PartitionSpec as P

F32, BF16 = jnp.float32, jnp.bfloat16
UNIT = 512

UNITS = 2
PER_LAYER = 16 // UNITS
CHUNKS = 6 * PER_LAYER
IN_VMEM = 2

S1 = 1
T = S1 + 2
LZ = 1
FIN = T + 3 * LZ
NEW = FIN + 1
GZ = NEW + 1
G1 = GZ + 3 * LZ
G0 = G1 + 2
END = G0 + 2

SLOTS = 32
OWN, CORE_SLOTS, FIRST_SLOTS, Z_SLOTS, LAST_SLOTS, SUMS = 4, 6, 4, 8, 8, 4


def kernel(*refs):
    g, w, m, v, out, m_out, v_out = (refs[i : i + 3] for i in range(0, 21, 3))
    own, core, first, zs, last, last_send, fresh, sums, kept, wb, mb, vb, mo, vo, local, recv, zrecv, grecv, sent, stored = refs[21:]

    rep, me = lax.axis_index("rep"), lax.axis_index("dp")
    c, z, y, x = lax.rem(me, 2), lax.rem(lax.div(me, 2), 4), lax.rem(lax.div(me, 8), 2), lax.div(me, 16)
    other = me + 1 - 2 * c
    xn, yn = me + 16 * (1 - 2 * x), me + 8 * (1 - 2 * y)

    def order(k):
        odd = lax.rem(k, 2)
        pn, qn = xn + odd * (yn - xn), yn + odd * (xn - yn)
        p, q = x + odd * (y - x), y + odd * (x - y)
        return pn, qn, p, q, 8 - 4 * odd, 4 + 4 * odd

    def by_weight(k, body):
        at = lax.div(k, PER_LAYER)
        which, layer, piece = lax.div(at, 2), lax.rem(at, 2), lax.rem(k, PER_LAYER)
        for i in range(3):
            pl.when(which == i)(functools.partial(body, i, layer, piece))

    def cut(i, piece, u=None):
        start, n = (piece * UNITS, UNITS) if u is None else (piece * UNITS + u, 1)
        if i < 2:
            return slice(None), pl.ds(pl.multiple_of(start * UNIT, UNIT), n * UNIT)
        return pl.ds(pl.multiple_of(start * 16, 16), n * 16), slice(None)

    def send(src, dst, s, r, to):
        pltpu.make_async_remote_copy(src, dst, s, r, device_id=(rep, to), device_id_type=pl.DeviceIdType.MESH).start()

    def wait(like, sem):
        pltpu.make_async_copy(like, like, sem).wait()

    def stage(t, offset, body):
        k = t - offset
        pl.when(jnp.logical_and(k >= 0, k < CHUNKS))(functools.partial(body, k))

    CORE, FIRST, LAST, NEXT, GATHER1, GATHER0, GATHERZ = range(7)

    def start(k):
        s, e, o = lax.rem(k, SLOTS), lax.rem(k, CORE_SLOTS), lax.rem(k, OWN)

        def body(i, layer, piece):
            for u in range(UNITS):
                rows, cols = cut(i, piece, u)
                send(g[i].at[layer, :, 1 - c, rows, cols], core.at[e, :, u], sent.at[CORE, s], recv.at[CORE, s], other)
                pltpu.make_async_copy(g[i].at[layer, :, c, rows, cols], own.at[o, :, u], local.at[o]).start()

        by_weight(k, body)

    def first_axis(k):
        s, e, f, o = lax.rem(k, SLOTS), lax.rem(k, CORE_SLOTS), lax.rem(k, FIRST_SLOTS), lax.rem(k, OWN)
        pn, _, p, _, sp, sq = order(k)
        wait(core.at[e], recv.at[CORE, s])
        wait(own.at[o], local.at[o])
        for q in range(2):
            j = (1 - p) * sp + q * sq

            @pl.loop(0, 4)
            def _(n):
                core[e, j + n] = (own[o, j + n].astype(F32) + core[e, j + n].astype(F32)).astype(BF16)

            send(core.at[e, pl.ds(j, 4)], first.at[f, q], sent.at[FIRST, s], recv.at[FIRST, s], pn)

    def sum_first(k):
        s, e, f, o, b = lax.rem(k, SLOTS), lax.rem(k, CORE_SLOTS), lax.rem(k, FIRST_SLOTS), lax.rem(k, OWN), lax.rem(k, SUMS)
        _, _, p, _, sp, sq = order(k)
        wait(first.at[f], recv.at[FIRST, s])
        for q in range(2):
            j = p * sp + q * sq

            @pl.loop(0, 4)
            def _(n):
                sums[b, n, q] = own[o, j + n].astype(F32) + core[e, j + n].astype(F32) + first[f, q, n].astype(F32)

    def hop(k, up):
        s, n, b = lax.rem(k, SLOTS), lax.rem(k, Z_SLOTS), lax.rem(k, SUMS)
        for to in (3, 2, 1) if up else (0, 1, 2):
            slot = to + 1 if up else to

            @pl.when(to > z if up else to < z)
            def _():
                @pl.when(z > 0 if up else z < 3)
                def _():
                    wait(zs.at[n, slot], zrecv.at[s, slot])
                    for q in range(2):
                        zs[n, slot, q] = (sums[b, to, q] + zs[n, slot, q].astype(F32)).astype(BF16)

                @pl.when(z == 0 if up else z == 3)
                def _():
                    for q in range(2):
                        zs[n, slot, q] = sums[b, to, q].astype(BF16)

                send(zs.at[n, slot], zs.at[n, slot], sent.at[GATHERZ + 1, s], zrecv.at[s, slot], me + 2 if up else me - 2)

    def finish(k):
        s, n, r, b, h = lax.rem(k, SLOTS), lax.rem(k, Z_SLOTS), lax.rem(k, LAST_SLOTS), lax.rem(k, SUMS), lax.rem(k, 2)
        _, qn, _, q, _, _ = order(k)

        @pl.when(z > 0)
        def _():
            wait(zs.at[n, z + 1], zrecv.at[s, z + 1])

        @pl.when(z < 3)
        def _():
            wait(zs.at[n, z], zrecv.at[s, z])

        @pl.when(z == 0)
        def _():
            last_send[r] = (sums[b, z, 1 - q] + zs[n, z, 1 - q].astype(F32)).astype(BF16)
            kept[h] = sums[b, z, q] + zs[n, z, q].astype(F32)

        @pl.when(z == 3)
        def _():
            last_send[r] = (sums[b, z, 1 - q] + zs[n, z + 1, 1 - q].astype(F32)).astype(BF16)
            kept[h] = sums[b, z, q] + zs[n, z + 1, q].astype(F32)

        @pl.when(jnp.logical_and(z > 0, z < 3))
        def _():
            last_send[r] = (sums[b, z, 1 - q] + zs[n, z, 1 - q].astype(F32) + zs[n, z + 1, 1 - q].astype(F32)).astype(BF16)
            kept[h] = sums[b, z, q] + zs[n, z, q].astype(F32) + zs[n, z + 1, q].astype(F32)

        send(last_send.at[r], last.at[r], sent.at[LAST, s], recv.at[LAST, s], qn)

        def load(i, layer, piece):
            for u in range(UNITS):
                rows, cols = cut(i, piece, u)
                pltpu.make_async_copy(w[i].at[layer, me, rows, cols], wb.at[h, u], local.at[OWN + h]).start()
                pltpu.make_async_copy(m[i].at[layer, rows, cols], mb.at[h, u], local.at[OWN + 2 + h]).start()
                pltpu.make_async_copy(v[i].at[layer, rows, cols], vb.at[h, u], local.at[OWN + 4 + h]).start()

        by_weight(k, load)

    def wait_stored(h):
        wait(mo.at[h], stored.at[h])
        wait(vo.at[h], stored.at[2 + h])

    def update(k):
        s, r, h = lax.rem(k, SLOTS), lax.rem(k, LAST_SLOTS), lax.rem(k, 2)
        _, qn, _, _, _, _ = order(k)
        wait(last.at[r], recv.at[LAST, s])
        wait(wb.at[h], local.at[OWN + h])
        wait(mb.at[h], local.at[OWN + 2 + h])
        wait(vb.at[h], local.at[OWN + 4 + h])
        pl.when(k >= 2)(functools.partial(wait_stored, h))
        grad = (kept[h] + last[r].astype(F32)).astype(BF16).astype(F32)
        old = wb[h].astype(F32)
        mm = 0.9 * mb[h] + 0.1 * grad
        vv = 0.95 * vb[h] + 0.05 * grad * grad
        mo[h] = mm
        vo[h] = vv
        new = (old - 0.02 * (mm * lax.rsqrt(vv + 1e-8) + 0.1 * old)).astype(BF16)

        def store(i, layer, piece):
            for u in range(UNITS):
                rows, cols = cut(i, piece, u)
                pltpu.make_async_copy(mo.at[h, u], m_out[i].at[layer, rows, cols], stored.at[h]).start()
                pltpu.make_async_copy(vo.at[h, u], v_out[i].at[layer, rows, cols], stored.at[2 + h]).start()
                here = out[i].at[layer, lax.div(me, 2), c, rows, cols]
                if i < IN_VMEM:
                    here[...] = new[u]
                else:
                    fresh[r, u] = new[u]
                    send(fresh.at[r, u], here, sent.at[NEXT, s], recv.at[NEXT, s], qn)
                    pltpu.make_async_copy(fresh.at[r, u], here, stored.at[4 + r]).start()
            if i < IN_VMEM:
                rows, cols = cut(i, piece)
                block = out[i].at[layer, lax.div(me, 2), c, rows, cols]
                send(block, block, sent.at[NEXT, s], recv.at[NEXT, s], qn)

        by_weight(k, store)

    def like(pieces):
        if pieces == 1:
            return out[0].at[0, 0, 0, :, pl.ds(0, UNITS * UNIT)]
        if pieces <= 16:
            return out[0].at[0, pl.ds(0, pieces), 0, :, pl.ds(0, UNITS * UNIT)]
        raise ValueError(pieces)

    def pass_on(k, at, up, down):
        s = lax.rem(k, SLOTS)
        _, _, p, _, sp, sq = order(k)

        def body(i, layer, piece):
            rows, cols = cut(i, piece)
            for cond, to in ((up, me + 2), (down, me - 2)):
                if cond is not None:

                    @pl.when(cond)
                    def _():
                        for q in range(2):
                            block = out[i].at[layer, p * sp + q * sq + at, c, rows, cols]
                            send(block, block, sent.at[GATHERZ, s], grecv.at[s, at], to)

        by_weight(k, body)

    def gather_own(k):
        s = lax.rem(k, SLOTS)
        wait(like(1), recv.at[NEXT, s])
        pl.when(k >= IN_VMEM * 2 * PER_LAYER)(lambda: wait(fresh.at[0], stored.at[4 + lax.rem(k, LAST_SLOTS)]))
        pass_on(k, z, z < 3, z > 0)

    def gather_z(k, d):
        s = lax.rem(k, SLOTS)

        @pl.when(z - d >= 0)
        def _():
            wait(like(2), grecv.at[s, z - d])
            if d < 3:
                pass_on(k, z - d, z < 3, None)

        @pl.when(z + d <= 3)
        def _():
            wait(like(2), grecv.at[s, z + d])
            if d < 3:
                pass_on(k, z + d, None, z > 0)

    def gather_first(k):
        s = lax.rem(k, SLOTS)
        pn, _, p, _, sp, sq = order(k)

        def body(i, layer, piece):
            rows, cols = cut(i, piece)
            for q in range(2):
                block = out[i].at[layer, pl.ds(p * sp + q * sq, 4), c, rows, cols]
                send(block, block, sent.at[GATHER1, s], recv.at[GATHER1, s], pn)

        by_weight(k, body)

    def gather_core(k):
        s = lax.rem(k, SLOTS)
        wait(like(8), recv.at[GATHER1, s])

        def body(i, layer, piece):
            rows, cols = cut(i, piece)
            block = out[i].at[layer, :, c, rows, cols]
            send(block, block, sent.at[GATHER0, s], recv.at[GATHER0, s], other)

        by_weight(k, body)

    def sent_first(k):
        s = lax.rem(k, SLOTS)
        wait(core.at[0], sent.at[CORE, s])
        wait(first.at[0], sent.at[FIRST, s])

    def sent_new(k):
        wait(like(1), sent.at[NEXT, lax.rem(k, SLOTS)])

    def sent_sums(k):
        s = lax.rem(k, SLOTS)
        wait(zs.at[0, pl.ds(0, 3)], sent.at[GATHERZ + 1, s])
        wait(last.at[0], sent.at[LAST, s])

    def end(k):
        s = lax.rem(k, SLOTS)
        wait(like(16), recv.at[GATHER0, s])
        pl.when(jnp.logical_or(z == 0, z == 3))(lambda: wait(like(2), sent.at[GATHERZ, s]))
        pl.when(jnp.logical_and(z > 0, z < 3))(lambda: wait(like(10), sent.at[GATHERZ, s]))
        wait(like(8), sent.at[GATHER1, s])
        wait(like(16), sent.at[GATHER0, s])

    @pl.loop(0, CHUNKS + END)
    def _(t):
        stage(t, END, end)
        stage(t, G0, gather_core)
        for d in (3, 2, 1):
            stage(t, GZ + d * LZ, functools.partial(gather_z, d=d))
        stage(t, G1, gather_first)
        stage(t, GZ, gather_own)
        stage(t, NEW, update)
        stage(t, NEW + 6, sent_new)
        stage(t, FIN + 3, sent_sums)
        stage(t, T + 2, sent_first)
        stage(t, FIN, finish)
        stage(t, T, sum_first)
        stage(t, T + LZ * z, functools.partial(hop, up=True))
        stage(t, T + LZ * (3 - z), functools.partial(hop, up=False))
        stage(t, S1, first_axis)
        stage(t, 0, start)

    for h in range(2):
        wait_stored(h)


def solution(mesh):
    n = (UNITS, 16, UNIT)

    def step(*arrays):
        g, w, m, v = (arrays[i : i + 3] for i in (0, 3, 6, 9))
        shapes = [one.shape for one in w]
        g = [one.reshape(2, 16, 2, one.shape[2] // 32, one.shape[3]) for one in g]
        w = [one.reshape(2, 32, one.shape[1] // 32, one.shape[2]) for one in w]
        results = pl.pallas_call(
            kernel,
            name="step",
            in_specs=[pl.BlockSpec(memory_space=pltpu.HBM)] * 12,
            out_specs=[pl.BlockSpec(memory_space=pltpu.VMEM)] * 2 + [pl.BlockSpec(memory_space=pltpu.HBM)] * 7,
            out_shape=[pltpu.VMEM(one.shape, BF16) for one in g[:2]] + [jax.ShapeDtypeStruct(g[2].shape, BF16)] + [jax.ShapeDtypeStruct(one.shape, F32) for one in (*m, *v)],
            scratch_shapes=[
                pltpu.VMEM((OWN, 16, *n), BF16),
                pltpu.VMEM((CORE_SLOTS, 16, *n), BF16),
                pltpu.VMEM((FIRST_SLOTS, 2, 4, *n), BF16),
                pltpu.VMEM((Z_SLOTS, 5, 2, *n), BF16),
                pltpu.VMEM((LAST_SLOTS, *n), BF16),
                pltpu.VMEM((LAST_SLOTS, *n), BF16),
                pltpu.VMEM((LAST_SLOTS, *n), BF16),
                pltpu.VMEM((SUMS, 4, 2, *n), F32),
                pltpu.VMEM((2, *n), F32),
                pltpu.VMEM((2, *n), BF16),
                pltpu.VMEM((2, *n), F32),
                pltpu.VMEM((2, *n), F32),
                pltpu.VMEM((2, *n), F32),
                pltpu.VMEM((2, *n), F32),
                pltpu.SemaphoreType.DMA((OWN + 6,)),
                pltpu.SemaphoreType.DMA((6, SLOTS)),
                pltpu.SemaphoreType.DMA((SLOTS, 5)),
                pltpu.SemaphoreType.DMA((SLOTS, 4)),
                pltpu.SemaphoreType.DMA((8, SLOTS)),
                pltpu.SemaphoreType.DMA((4 + LAST_SLOTS,)),
            ],
            compiler_params=pltpu.CompilerParams(has_side_effects=True, vmem_limit_bytes=16 * 2**20),
        )(*g, *w, *m, *v)
        return (*(one.reshape(shape) for one, shape in zip(results[:3], shapes, strict=True)), *results[3:])

    all_of, cut = P(None, None, None), P(None, "dp", None)
    return jax.shard_map(
        step,
        mesh=mesh,
        in_specs=(P(("rep", "dp"), None, None, None),) * 3 + (all_of,) * 3 + (cut,) * 6,
        out_specs=(P("rep", None, None),) * 3 + (P("rep", "dp", None),) * 6,
        check_vma=False,
    )
```

```python
import functools

import jax
import jax.numpy as jnp
from jax import lax
from jax.experimental import pallas as pl
from jax.experimental.pallas import tpu as pltpu
from jax.sharding import PartitionSpec as P

F32, BF16 = jnp.float32, jnp.bfloat16
UNIT = 512

UNITS = 1
PER_LAYER = 16 // UNITS
CHUNKS = 6 * PER_LAYER
VMEM_MIB = 16
IN_VMEM = 2

S1 = 2
T = S1 + 3
LZ = 2
FIN = T + 3 * LZ
NEW = FIN + 2
GZ = NEW + 2
G1 = GZ + 3 * LZ
G0 = G1 + 3
END = G0 + 2

SLOTS = 32
OWN, CORE_SLOTS, FIRST_SLOTS, Z_SLOTS, LAST_SLOTS, SUMS = 8, 16, 8, 16, 16, 8


def kernel(*refs):
    g, w, m, v, out, m_out, v_out = (refs[i : i + 3] for i in range(0, 21, 3))
    own, core, first, zs, last, last_send, fresh, sums, kept, *held = refs[21:33]
    whole, local, recv, zrecv, grecv, sent, stored = refs[33:]

    rep, me = lax.axis_index("rep"), lax.axis_index("dp")
    c, z, y, x = lax.rem(me, 2), lax.rem(lax.div(me, 2), 4), lax.rem(lax.div(me, 8), 2), lax.div(me, 16)
    other = me + 1 - 2 * c
    across = (me + 16 * (1 - 2 * x), me + 8 * (1 - 2 * y))

    def pair(odd, p, *rest):
        return (slice(None), p, *rest) if odd else (p, slice(None), *rest)

    def by_weight(k, body):
        at = lax.div(k, PER_LAYER)
        which, layer, piece = lax.div(at, 2), lax.rem(at, 2), lax.rem(k, PER_LAYER)
        for i in range(3):
            pl.when(which == i)(functools.partial(body, i, layer, piece))

    def cut(i, piece, u=None):
        start, n = (piece * UNITS, UNITS) if u is None else (piece * UNITS + u, 1)
        if i < 2:
            return slice(None), pl.ds(pl.multiple_of(start * UNIT, UNIT), n * UNIT)
        return pl.ds(pl.multiple_of(start * 16, 16), n * 16), slice(None)

    def send(src, dst, s, r, to):
        pltpu.make_async_remote_copy(src, dst, s, r, device_id=(rep, to), device_id_type=pl.DeviceIdType.MESH).start()

    def wait(like, sem):
        pltpu.make_async_copy(like, like, sem).wait()

    CORE, FIRST, LAST, NEXT, GATHER1, GATHER0, GATHERZ, SUMZ = range(8)
    every = slice(None)

    loads = [pltpu.make_async_copy(a, b, whole.at[i]) for i, (a, b) in enumerate(zip((*m, *v), (*m_out, *v_out), strict=True))]
    loads += [pltpu.make_async_copy(w[i].at[:, me], held[i], whole.at[6 + i]) for i in range(3)]

    def start(k, odd):
        s, e, o = lax.rem(k, SLOTS), lax.rem(k, CORE_SLOTS), lax.rem(k, OWN)

        def body(i, layer, piece):
            for u in range(UNITS):
                rows, cols = cut(i, piece, u)
                send(g[i].at[layer, :, :, :, 1 - c, rows, cols], core.at[e, :, :, :, u], sent.at[CORE, s], recv.at[CORE, s], other)
                pltpu.make_async_copy(g[i].at[layer, :, :, :, c, rows, cols], own.at[o, :, :, :, u], local.at[o]).start()

        by_weight(k, body)

    def first_axis(k, odd):
        s, e, f, o = lax.rem(k, SLOTS), lax.rem(k, CORE_SLOTS), lax.rem(k, FIRST_SLOTS), lax.rem(k, OWN)
        p = 1 - (y if odd else x)
        wait(core.at[e], recv.at[CORE, s])
        wait(own.at[o], local.at[o])

        @pl.loop(0, 4)
        def _(n):
            at = pair(odd, p, n)
            core[e, *at] = (own[o, *at].astype(F32) + core[e, *at].astype(F32)).astype(BF16)

        send(core.at[e, *pair(odd, p)], first.at[f], sent.at[FIRST, s], recv.at[FIRST, s], across[odd])

    def sum_first(k, odd):
        s, e, f, o, b = lax.rem(k, SLOTS), lax.rem(k, CORE_SLOTS), lax.rem(k, FIRST_SLOTS), lax.rem(k, OWN), lax.rem(k, SUMS)
        p = y if odd else x
        wait(first.at[f], recv.at[FIRST, s])

        @pl.loop(0, 4)
        def _(n):
            at = pair(odd, p, n)
            sums[b, n] = own[o, *at].astype(F32) + core[e, *at].astype(F32) + first[f, :, n].astype(F32)

    def hop(k, up):
        s, n, b = lax.rem(k, SLOTS), lax.rem(k, Z_SLOTS), lax.rem(k, SUMS)
        for to in (3, 2, 1) if up else (0, 1, 2):
            slot = to + 1 if up else to

            @pl.when(to > z if up else to < z)
            def _():
                @pl.when(z > 0 if up else z < 3)
                def _():
                    wait(zs.at[n, slot], zrecv.at[s, slot])
                    zs[n, slot] = (sums[b, to] + zs[n, slot].astype(F32)).astype(BF16)

                @pl.when(z == 0 if up else z == 3)
                def _():
                    zs[n, slot] = sums[b, to].astype(BF16)

                send(zs.at[n, slot], zs.at[n, slot], sent.at[SUMZ, s], zrecv.at[s, slot], me + 2 if up else me - 2)

    def finish(k, odd):
        s, n, r, b, h = lax.rem(k, SLOTS), lax.rem(k, Z_SLOTS), lax.rem(k, LAST_SLOTS), lax.rem(k, SUMS), lax.rem(k, 2)
        q = x if odd else y

        @pl.when(z > 0)
        def _():
            wait(zs.at[n, z + 1], zrecv.at[s, z + 1])

        @pl.when(z < 3)
        def _():
            wait(zs.at[n, z], zrecv.at[s, z])

        def put_total(*slots):
            for to in (1 - q, q):
                total = sums[b, z, to]
                for slot in slots:
                    total = total + zs[n, slot, to].astype(F32)
                if to is q:
                    kept[h] = total
                else:
                    last_send[r] = total.astype(BF16)

        pl.when(z == 0)(lambda: put_total(z))
        pl.when(z == 3)(lambda: put_total(z + 1))
        pl.when(jnp.logical_and(z > 0, z < 3))(lambda: put_total(z, z + 1))
        send(last_send.at[r], last.at[r], sent.at[LAST, s], recv.at[LAST, s], across[1 - odd])

    def update(k, odd):
        s, r, h = lax.rem(k, SLOTS), lax.rem(k, LAST_SLOTS), lax.rem(k, 2)

        @pl.when(k == 0)
        def _():
            for one in loads:
                one.wait()

        wait(last.at[r], recv.at[LAST, s])

        def store(i, layer, piece):
            for u in range(UNITS):
                rows, cols = cut(i, piece, u)
                grad = (kept[h, u] + last[r, u].astype(F32)).astype(BF16).astype(F32)
                old = held[i][layer, rows, cols].astype(F32)
                mm = 0.9 * m_out[i][layer, rows, cols] + 0.1 * grad
                vv = 0.95 * v_out[i][layer, rows, cols] + 0.05 * grad * grad
                m_out[i][layer, rows, cols] = mm
                v_out[i][layer, rows, cols] = vv
                new = (old - 0.02 * (mm * lax.rsqrt(vv + 1e-8) + 0.1 * old)).astype(BF16)
                here = out[i].at[layer, x, y, z, c, rows, cols]
                if i < IN_VMEM:
                    here[...] = new
                else:
                    fresh[r, u] = new
                    send(fresh.at[r, u], here, sent.at[NEXT, s], recv.at[NEXT, s], across[1 - odd])
                    pltpu.make_async_copy(fresh.at[r, u], here, stored.at[r]).start()
            if i < IN_VMEM:
                block = out[i].at[layer, x, y, z, c, *cut(i, piece)]
                send(block, block, sent.at[NEXT, s], recv.at[NEXT, s], across[1 - odd])

        by_weight(k, store)

    def like(pieces):
        if pieces == 1:
            return last.at[0]
        return zs.at[0] if pieces == 10 else zs.at[0, 0] if pieces == 2 else first.at[0] if pieces == 8 else core.at[0]

    def push(k, to, s, r, *at):
        def body(i, layer, piece):
            block = out[i].at[layer, *at, c, *cut(i, piece)]
            send(block, block, s, r, to)

        by_weight(k, body)

    def pass_on(k, odd, at, up):
        s = lax.rem(k, SLOTS)
        push(k, me + 2 if up else me - 2, sent.at[GATHERZ, s], grecv.at[s, at], *pair(odd, y if odd else x, at))

    def gather_own(k, odd):
        pl.when(k >= IN_VMEM * 2 * PER_LAYER)(lambda: wait(fresh.at[0], stored.at[lax.rem(k, LAST_SLOTS)]))
        wait(like(1), recv.at[NEXT, lax.rem(k, SLOTS)])
        pl.when(z < 3)(lambda: pass_on(k, odd, z, True))
        pl.when(z > 0)(lambda: pass_on(k, odd, z, False))

    def gather_z(k, odd, d):
        s = lax.rem(k, SLOTS)

        @pl.when(z - d >= 0)
        def _():
            wait(like(2), grecv.at[s, z - d])
            if d < 3:
                pl.when(z < 3)(lambda: pass_on(k, odd, z - d, True))

        @pl.when(z + d <= 3)
        def _():
            wait(like(2), grecv.at[s, z + d])
            if d < 3:
                pl.when(z > 0)(lambda: pass_on(k, odd, z + d, False))

    def gather_first(k, odd):
        s = lax.rem(k, SLOTS)
        push(k, across[odd], sent.at[GATHER1, s], recv.at[GATHER1, s], *pair(odd, y if odd else x, every))

    def gather_core(k, odd):
        s = lax.rem(k, SLOTS)
        wait(like(8), recv.at[GATHER1, s])
        push(k, other, sent.at[GATHER0, s], recv.at[GATHER0, s], every, every, every)

    def sent_first(k, odd):
        s = lax.rem(k, SLOTS)
        wait(core.at[0], sent.at[CORE, s])
        wait(first.at[0], sent.at[FIRST, s])

    def sent_sums(k, odd):
        s = lax.rem(k, SLOTS)
        wait(zs.at[0, pl.ds(0, 3)], sent.at[SUMZ, s])
        wait(last.at[0], sent.at[LAST, s])

    def end(k, odd):
        s = lax.rem(k, SLOTS)
        wait(like(16), recv.at[GATHER0, s])
        wait(like(1), sent.at[NEXT, s])
        pl.when(jnp.logical_or(z == 0, z == 3))(lambda: wait(like(2), sent.at[GATHERZ, s]))
        pl.when(jnp.logical_and(z > 0, z < 3))(lambda: wait(like(10), sent.at[GATHERZ, s]))
        wait(like(8), sent.at[GATHER1, s])
        wait(like(16), sent.at[GATHER0, s])

    def stage(t, half, offset, body):
        k = t - offset
        pl.when(jnp.logical_and(k >= 0, k < CHUNKS))(functools.partial(body, k, (half - offset) % 2) if isinstance(offset, int) else functools.partial(body, k))

    def tick(t, half):
        at = functools.partial(stage, t, half)
        at(END, end)
        at(G0, gather_core)
        for d in (3, 2, 1):
            at(GZ + d * LZ, functools.partial(gather_z, d=d))
        at(G1, gather_first)
        at(GZ, gather_own)
        at(NEW, update)
        at(FIN + 3, sent_sums)
        at(T + 2, sent_first)
        at(FIN, finish)
        at(T, sum_first)
        at(T + LZ * z, functools.partial(hop, up=True))
        at(T + LZ * (3 - z), functools.partial(hop, up=False))
        at(S1, first_axis)
        at(0, start)

    @pl.loop(0, (CHUNKS + END + 1) // 2)
    def _(i):
        tick(2 * i, 0)

        @pl.when(i == 0)
        def _():
            for one in loads:
                one.start()

        tick(2 * i + 1, 1)


def put(*refs):
    copies = [pltpu.make_async_copy(refs[i], refs[6 + i], refs[12].at[i]) for i in range(6)]
    for one in copies:
        one.start()
    for one in copies:
        one.wait()


def solution(mesh):
    n = (UNITS, 16, UNIT)

    def step(*arrays):
        g, w, m, v = (arrays[i : i + 3] for i in (0, 3, 6, 9))
        shapes = [one.shape for one in w]
        g = [one.reshape(2, 2, 2, 4, 2, one.shape[2] // 32, one.shape[3]) for one in g]
        w = [one.reshape(2, 32, one.shape[1] // 32, one.shape[2]) for one in w]
        results = pl.pallas_call(
            kernel,
            name="step",
            in_specs=[pl.BlockSpec(memory_space=pltpu.HBM)] * 12,
            out_specs=[pl.BlockSpec(memory_space=pltpu.HBM if IN_VMEM <= i < 3 else pltpu.VMEM) for i in range(9)],
            out_shape=[pltpu.VMEM(one.shape, BF16) if i < IN_VMEM else jax.ShapeDtypeStruct(one.shape, BF16) for i, one in enumerate(g)]
            + [pltpu.VMEM(one.shape, F32) for one in (*m, *v)],
            scratch_shapes=[
                pltpu.VMEM((OWN, 2, 2, 4, *n), BF16),
                pltpu.VMEM((CORE_SLOTS, 2, 2, 4, *n), BF16),
                pltpu.VMEM((FIRST_SLOTS, 2, 4, *n), BF16),
                pltpu.VMEM((Z_SLOTS, 5, 2, *n), BF16),
                pltpu.VMEM((LAST_SLOTS, *n), BF16),
                pltpu.VMEM((LAST_SLOTS, *n), BF16),
                pltpu.VMEM((LAST_SLOTS, *n), BF16),
                pltpu.VMEM((SUMS, 4, 2, *n), F32),
                pltpu.VMEM((2, *n), F32),
                *(pltpu.VMEM(one.shape, BF16) for one in m),
                pltpu.SemaphoreType.DMA((9,)),
                pltpu.SemaphoreType.DMA((OWN,)),
                pltpu.SemaphoreType.DMA((6, SLOTS)),
                pltpu.SemaphoreType.DMA((SLOTS, 5)),
                pltpu.SemaphoreType.DMA((SLOTS, 4)),
                pltpu.SemaphoreType.DMA((8, SLOTS)),
                pltpu.SemaphoreType.DMA((LAST_SLOTS,)),
            ],
            compiler_params=pltpu.CompilerParams(has_side_effects=True, vmem_limit_bytes=VMEM_MIB * 2**20),
        )(*g, *w, *m, *v)
        moments = pl.pallas_call(
            put,
            name="put",
            in_specs=[pl.BlockSpec(memory_space=pltpu.VMEM)] * 6,
            out_specs=[pl.BlockSpec(memory_space=pl.ANY)] * 6,
            out_shape=[jax.ShapeDtypeStruct(one.shape, one.dtype) for one in results[3:]],
            scratch_shapes=[pltpu.SemaphoreType.DMA((6,))],
            compiler_params=pltpu.CompilerParams(vmem_limit_bytes=2**20),
        )(*results[3:])
        return (*(one.reshape(shape) for one, shape in zip(results[:3], shapes, strict=True)), *moments)

    all_of, cut = P(None, None, None), P(None, "dp", None)
    return jax.shard_map(
        step,
        mesh=mesh,
        in_specs=(P(("rep", "dp"), None, None, None),) * 3 + (all_of,) * 3 + (cut,) * 6,
        out_specs=(P("rep", None, None),) * 3 + (P("rep", "dp", None),) * 6,
        check_vma=False,
    )
```

```python
import functools

import jax
import jax.numpy as jnp
from jax import lax
from jax.experimental import pallas as pl
from jax.experimental.pallas import tpu as pltpu
from jax.sharding import PartitionSpec as P

F32, BF16 = jnp.float32, jnp.bfloat16
UNIT = 512

UNITS = 1
PER_LAYER = 16 // UNITS
CHUNKS = 6 * PER_LAYER
VMEM_MIB = 16
IN_VMEM = 2

S1 = 2
T = S1 + 3
LZ = 2
FIN = T + 3 * LZ
NEW = FIN + 2
GZ = NEW + 2
G1 = GZ + 3 * LZ
G0 = G1 + 3
END = G0 + 2

SLOTS = 32
OWN, CORE_SLOTS, FIRST_SLOTS, Z_SLOTS, LAST_SLOTS, SUMS = 8, 16, 8, 16, 16, 8


def kernel(*refs):
    g, w, m, v, out, m_out, v_out = (refs[i : i + 3] for i in range(0, 21, 3))
    own, core, first, zs, last, last_send, fresh, sums, kept, *held = refs[21:33]
    whole, local, recv, zrecv, grecv, sent, stored = refs[33:]

    rep, me = lax.axis_index("rep"), lax.axis_index("dp")
    c, z, y, x = lax.rem(me, 2), lax.rem(lax.div(me, 2), 4), lax.rem(lax.div(me, 8), 2), lax.div(me, 16)
    other = me + 1 - 2 * c
    across = (me + 16 * (1 - 2 * x), me + 8 * (1 - 2 * y))

    def pair(odd, p, *rest):
        return (slice(None), p, *rest) if odd else (p, slice(None), *rest)

    def by_weight(k, body):
        at = lax.div(k, PER_LAYER)
        which, layer, piece = lax.div(at, 2), lax.rem(at, 2), lax.rem(k, PER_LAYER)
        for i in range(3):
            pl.when(which == i)(functools.partial(body, i, layer, piece))

    def cut(i, piece, u=None):
        start, n = (piece * UNITS, UNITS) if u is None else (piece * UNITS + u, 1)
        if i < 2:
            return slice(None), pl.ds(pl.multiple_of(start * UNIT, UNIT), n * UNIT)
        return pl.ds(pl.multiple_of(start * 16, 16), n * 16), slice(None)

    def send(src, dst, s, r, to):
        pltpu.make_async_remote_copy(src, dst, s, r, device_id=(rep, to), device_id_type=pl.DeviceIdType.MESH).start()

    def wait(like, sem):
        pltpu.make_async_copy(like, like, sem).wait()

    CORE, FIRST, LAST, NEXT, GATHER1, GATHER0, GATHERZ, SUMZ = range(8)
    every = slice(None)

    loads = [pltpu.make_async_copy(a, b, whole.at[i]) for i, (a, b) in enumerate(zip((*m, *v), (*m_out, *v_out), strict=True))]
    loads += [pltpu.make_async_copy(w[i].at[:, me], held[i], whole.at[6 + i]) for i in range(3)]

    def start(k, odd):
        s, e, o = lax.rem(k, SLOTS), lax.rem(k, CORE_SLOTS), lax.rem(k, OWN)

        def body(i, layer, piece):
            for u in range(UNITS):
                rows, cols = cut(i, piece, u)
                send(g[i].at[layer, :, :, :, 1 - c, rows, cols], core.at[e, :, :, :, u], sent.at[CORE, s], recv.at[CORE, s], other)
                pltpu.make_async_copy(g[i].at[layer, :, :, :, c, rows, cols], own.at[o, :, :, :, u], local.at[o]).start()

        by_weight(k, body)

    def first_axis(k, odd):
        s, e, f, o = lax.rem(k, SLOTS), lax.rem(k, CORE_SLOTS), lax.rem(k, FIRST_SLOTS), lax.rem(k, OWN)
        p = 1 - (y if odd else x)
        wait(core.at[e], recv.at[CORE, s])
        wait(own.at[o], local.at[o])

        @pl.loop(0, 4, unroll=True)
        def _(n):
            at = pair(odd, p, n)
            core[e, *at] = (own[o, *at].astype(F32) + core[e, *at].astype(F32)).astype(BF16)

        send(core.at[e, *pair(odd, p)], first.at[f], sent.at[FIRST, s], recv.at[FIRST, s], across[odd])

    def sum_first(k, odd):
        s, e, f, o, b = lax.rem(k, SLOTS), lax.rem(k, CORE_SLOTS), lax.rem(k, FIRST_SLOTS), lax.rem(k, OWN), lax.rem(k, SUMS)
        p = y if odd else x
        wait(first.at[f], recv.at[FIRST, s])

        @pl.loop(0, 4, unroll=True)
        def _(n):
            at = pair(odd, p, n)
            sums[b, n] = own[o, *at].astype(F32) + core[e, *at].astype(F32) + first[f, :, n].astype(F32)

    def hop(k, up):
        s, n, b = lax.rem(k, SLOTS), lax.rem(k, Z_SLOTS), lax.rem(k, SUMS)
        for to in (3, 2, 1) if up else (0, 1, 2):
            slot = to + 1 if up else to

            @pl.when(to > z if up else to < z)
            def _():
                @pl.when(z > 0 if up else z < 3)
                def _():
                    wait(zs.at[n, slot], zrecv.at[s, slot])
                    zs[n, slot] = (sums[b, to] + zs[n, slot].astype(F32)).astype(BF16)

                @pl.when(z == 0 if up else z == 3)
                def _():
                    zs[n, slot] = sums[b, to].astype(BF16)

                send(zs.at[n, slot], zs.at[n, slot], sent.at[SUMZ, s], zrecv.at[s, slot], me + 2 if up else me - 2)

    def finish(k, odd):
        s, n, r, b, h = lax.rem(k, SLOTS), lax.rem(k, Z_SLOTS), lax.rem(k, LAST_SLOTS), lax.rem(k, SUMS), lax.rem(k, 2)
        q = x if odd else y

        @pl.when(z > 0)
        def _():
            wait(zs.at[n, z + 1], zrecv.at[s, z + 1])

        @pl.when(z < 3)
        def _():
            wait(zs.at[n, z], zrecv.at[s, z])

        def put_total(*slots):
            for to in (1 - q, q):
                total = sums[b, z, to]
                for slot in slots:
                    total = total + zs[n, slot, to].astype(F32)
                if to is q:
                    kept[h] = total
                else:
                    last_send[r] = total.astype(BF16)

        pl.when(z == 0)(lambda: put_total(z))
        pl.when(z == 3)(lambda: put_total(z + 1))
        pl.when(jnp.logical_and(z > 0, z < 3))(lambda: put_total(z, z + 1))
        send(last_send.at[r], last.at[r], sent.at[LAST, s], recv.at[LAST, s], across[1 - odd])

    def update(k, odd):
        s, r, h = lax.rem(k, SLOTS), lax.rem(k, LAST_SLOTS), lax.rem(k, 2)

        @pl.when(k == 0)
        def _():
            for one in loads:
                one.wait()

        wait(last.at[r], recv.at[LAST, s])

        def store(i, layer, piece):
            for u in range(UNITS):
                rows, cols = cut(i, piece, u)
                grad = (kept[h, u] + last[r, u].astype(F32)).astype(BF16).astype(F32)
                old = held[i][layer, rows, cols].astype(F32)
                mm = 0.9 * m_out[i][layer, rows, cols] + 0.1 * grad
                vv = 0.95 * v_out[i][layer, rows, cols] + 0.05 * grad * grad
                m_out[i][layer, rows, cols] = mm
                v_out[i][layer, rows, cols] = vv
                new = (old - 0.02 * (mm * lax.rsqrt(vv + 1e-8) + 0.1 * old)).astype(BF16)
                here = out[i].at[layer, x, y, z, c, rows, cols]
                if i < IN_VMEM:
                    here[...] = new
                else:
                    fresh[r, u] = new
                    send(fresh.at[r, u], here, sent.at[NEXT, s], recv.at[NEXT, s], across[1 - odd])
                    pltpu.make_async_copy(fresh.at[r, u], here, stored.at[r]).start()
            if i < IN_VMEM:
                block = out[i].at[layer, x, y, z, c, *cut(i, piece)]
                send(block, block, sent.at[NEXT, s], recv.at[NEXT, s], across[1 - odd])

        by_weight(k, store)

    def like(pieces):
        if pieces == 1:
            return last.at[0]
        return zs.at[0] if pieces == 10 else zs.at[0, 0] if pieces == 2 else first.at[0] if pieces == 8 else core.at[0]

    def push(k, to, s, r, *at):
        def body(i, layer, piece):
            block = out[i].at[layer, *at, c, *cut(i, piece)]
            send(block, block, s, r, to)

        by_weight(k, body)

    def pass_on(k, odd, at, up):
        s = lax.rem(k, SLOTS)
        push(k, me + 2 if up else me - 2, sent.at[GATHERZ, s], grecv.at[s, at], *pair(odd, y if odd else x, at))

    def gather_own(k, odd):
        pl.when(k >= IN_VMEM * 2 * PER_LAYER)(lambda: wait(fresh.at[0], stored.at[lax.rem(k, LAST_SLOTS)]))
        wait(like(1), recv.at[NEXT, lax.rem(k, SLOTS)])
        pl.when(z < 3)(lambda: pass_on(k, odd, z, True))
        pl.when(z > 0)(lambda: pass_on(k, odd, z, False))

    def gather_z(k, odd, d):
        s = lax.rem(k, SLOTS)

        @pl.when(z - d >= 0)
        def _():
            wait(like(2), grecv.at[s, z - d])
            if d < 3:
                pl.when(z < 3)(lambda: pass_on(k, odd, z - d, True))

        @pl.when(z + d <= 3)
        def _():
            wait(like(2), grecv.at[s, z + d])
            if d < 3:
                pl.when(z > 0)(lambda: pass_on(k, odd, z + d, False))

    def gather_first(k, odd):
        s = lax.rem(k, SLOTS)
        push(k, across[odd], sent.at[GATHER1, s], recv.at[GATHER1, s], *pair(odd, y if odd else x, every))

    def gather_core(k, odd):
        s = lax.rem(k, SLOTS)
        wait(like(8), recv.at[GATHER1, s])
        push(k, other, sent.at[GATHER0, s], recv.at[GATHER0, s], every, every, every)

    def sent_first(k, odd):
        s = lax.rem(k, SLOTS)
        wait(core.at[0], sent.at[CORE, s])
        wait(first.at[0], sent.at[FIRST, s])

    def sent_sums(k, odd):
        s = lax.rem(k, SLOTS)
        wait(zs.at[0, pl.ds(0, 3)], sent.at[SUMZ, s])
        wait(last.at[0], sent.at[LAST, s])

    def end(k, odd):
        s = lax.rem(k, SLOTS)
        wait(like(16), recv.at[GATHER0, s])
        wait(like(1), sent.at[NEXT, s])
        pl.when(jnp.logical_or(z == 0, z == 3))(lambda: wait(like(2), sent.at[GATHERZ, s]))
        pl.when(jnp.logical_and(z > 0, z < 3))(lambda: wait(like(10), sent.at[GATHERZ, s]))
        wait(like(8), sent.at[GATHER1, s])
        wait(like(16), sent.at[GATHER0, s])

    def stage(t, half, offset, body):
        k = t - offset
        pl.when(jnp.logical_and(k >= 0, k < CHUNKS))(functools.partial(body, k, (half - offset) % 2) if isinstance(offset, int) else functools.partial(body, k))

    def tick(t, half):
        at = functools.partial(stage, t, half)
        at(END, end)
        for d in (3, 2, 1):
            at(GZ + d * LZ, functools.partial(gather_z, d=d))
        at(G1, gather_first)
        at(GZ, gather_own)
        at(NEW, update)
        at(FIN + 3, sent_sums)
        at(T + 2, sent_first)
        at(FIN, finish)
        at(T, sum_first)
        at(T + LZ * z, functools.partial(hop, up=True))
        at(T + LZ * (3 - z), functools.partial(hop, up=False))
        at(S1, first_axis)
        at(G0, gather_core)
        at(0, start)

    @pl.loop(0, (CHUNKS + END + 1) // 2)
    def _(i):
        tick(2 * i, 0)

        @pl.when(i == 0)
        def _():
            for one in loads:
                one.start()

        tick(2 * i + 1, 1)


def put(*refs):
    copies = [pltpu.make_async_copy(refs[i], refs[6 + i], refs[12].at[i]) for i in range(6)]
    for one in copies:
        one.start()
    for one in copies:
        one.wait()


def solution(mesh):
    n = (UNITS, 16, UNIT)

    def step(*arrays):
        g, w, m, v = (arrays[i : i + 3] for i in (0, 3, 6, 9))
        shapes = [one.shape for one in w]
        g = [one.reshape(2, 2, 2, 4, 2, one.shape[2] // 32, one.shape[3]) for one in g]
        w = [one.reshape(2, 32, one.shape[1] // 32, one.shape[2]) for one in w]
        results = pl.pallas_call(
            kernel,
            name="step",
            in_specs=[pl.BlockSpec(memory_space=pltpu.HBM)] * 12,
            out_specs=[pl.BlockSpec(memory_space=pltpu.HBM if IN_VMEM <= i < 3 else pltpu.VMEM) for i in range(9)],
            out_shape=[pltpu.VMEM(one.shape, BF16) if i < IN_VMEM else jax.ShapeDtypeStruct(one.shape, BF16) for i, one in enumerate(g)]
            + [pltpu.VMEM(one.shape, F32) for one in (*m, *v)],
            scratch_shapes=[
                pltpu.VMEM((OWN, 2, 2, 4, *n), BF16),
                pltpu.VMEM((CORE_SLOTS, 2, 2, 4, *n), BF16),
                pltpu.VMEM((FIRST_SLOTS, 2, 4, *n), BF16),
                pltpu.VMEM((Z_SLOTS, 5, 2, *n), BF16),
                pltpu.VMEM((LAST_SLOTS, *n), BF16),
                pltpu.VMEM((LAST_SLOTS, *n), BF16),
                pltpu.VMEM((LAST_SLOTS, *n), BF16),
                pltpu.VMEM((SUMS, 4, 2, *n), F32),
                pltpu.VMEM((2, *n), F32),
                *(pltpu.VMEM(one.shape, BF16) for one in m),
                pltpu.SemaphoreType.DMA((9,)),
                pltpu.SemaphoreType.DMA((OWN,)),
                pltpu.SemaphoreType.DMA((6, SLOTS)),
                pltpu.SemaphoreType.DMA((SLOTS, 5)),
                pltpu.SemaphoreType.DMA((SLOTS, 4)),
                pltpu.SemaphoreType.DMA((8, SLOTS)),
                pltpu.SemaphoreType.DMA((LAST_SLOTS,)),
            ],
            compiler_params=pltpu.CompilerParams(has_side_effects=True, vmem_limit_bytes=VMEM_MIB * 2**20),
        )(*g, *w, *m, *v)
        moments = pl.pallas_call(
            put,
            name="put",
            in_specs=[pl.BlockSpec(memory_space=pltpu.VMEM)] * 6,
            out_specs=[pl.BlockSpec(memory_space=pl.ANY)] * 6,
            out_shape=[jax.ShapeDtypeStruct(one.shape, one.dtype) for one in results[3:]],
            scratch_shapes=[pltpu.SemaphoreType.DMA((6,))],
            compiler_params=pltpu.CompilerParams(vmem_limit_bytes=2**20),
        )(*results[3:])
        return (*(one.reshape(shape) for one, shape in zip(results[:3], shapes, strict=True)), *moments)

    all_of, cut = P(None, None, None), P(None, "dp", None)
    return jax.shard_map(
        step,
        mesh=mesh,
        in_specs=(P(("rep", "dp"), None, None, None),) * 3 + (all_of,) * 3 + (cut,) * 6,
        out_specs=(P("rep", None, None),) * 3 + (P("rep", "dp", None),) * 6,
        check_vma=False,
    )
```
